32 devices in a mesh: tm: 8 (over z, y), space: 4 (over x, core).
Axes of the slice: x: 2, y: 2, z: 4, core: 2. Of those that a mesh axis runs over, the one named last changes fastest.
Arguments:
- observed: float32 [64, 512, 128], P('tm', 'space'), may hold values from -6 to 6
- gain: float32 [4, 128, 128], P('space'), may hold values from -0.15625 to 0.15625
- trans: float32 [4, 384, 128], P('space'), may hold values from -1 to 1
- dynamics: float32 [4, 384, 128], P('space'), may hold values from -1 to 1
- smooth_gain: float32 [4, 384, 128], P('space'), may hold values from -1 to 1
Outputs:
- filtered: float32 [64, 512, 128], P('tm', 'space')
- smoothed: float32 [64, 512, 128], P('tm', 'space')
The draws below stay inside these ranges and needn't reach their ends.
All inputs are finite; a program needn't handle non-finite values.
Results may differ from the reference program's by a relative error of at most 0.00017.
Values sent between devices are 32-bit elements; how exact they have to be, the bound alone decides.
A program may use at most 128 MiB of HBM per device.

```python
import jax
import jax.numpy as jnp
from jax import lax

TILE = 128
MEMBERS = 128
STEPS = 64
STATE = 512
N_SPACE = 4


def banded_draw(key, slow_share):
    count_tiles = STATE // TILE
    key_noise, key_rate, key_pick = jax.random.split(key, 3)
    noise = jax.random.normal(key_noise, (count_tiles, 3 * TILE, TILE), jnp.float32) * (0.05 / (3 * TILE))
    picks = jax.random.uniform(key_pick, (count_tiles, TILE), jnp.float32)
    levels = jax.random.uniform(key_rate, (count_tiles, TILE), jnp.float32)
    slow = 0.993 + 0.005 * levels
    fast = 0.5 + 0.45 * levels
    rates = jnp.where(picks < slow_share, slow, fast)
    diagonal = jnp.eye(TILE, dtype=jnp.float32)[None] * rates[:, None, :]
    coupling = 0.25
    upper = noise[:, :TILE, :] + coupling * diagonal
    middle = noise[:, TILE:2 * TILE, :] + (1.0 - 2.0 * coupling) * diagonal
    lower = noise[:, 2 * TILE:, :] + coupling * diagonal
    return jnp.concatenate([upper, middle, lower], 1)


def draw_trans(key, part):
    return banded_draw(jax.random.fold_in(key, 11), 0.5)


def draw_dynamics(key, part):
    return banded_draw(jax.random.fold_in(key, 23), 0.5)


def draw_smooth_gain(key, part):
    return banded_draw(jax.random.fold_in(key, 37), 0.5)


def level_of(stream_key, dims, cuts, smallest, high):
    def one(dim, shards_of):
        draws = jax.random.uniform(jax.random.fold_in(jax.random.fold_in(stream_key, 6), dim), (shards_of,), jnp.float32, smallest / len(cuts), high / len(cuts))
        return jnp.repeat(jnp.exp(draws), dims[dim] // shards_of).reshape((-1,) + (1,) * (len(dims) - dim - 1))

    level = one(*cuts[0])
    for cut in cuts[1:]:
        level = level * one(*cut)
    return level


def scatter_about(rng, dims, scale, most, cuts=(), held_as=jnp.bfloat16):
    array = jax.random.normal(rng, dims, jnp.float32) * scale
    if len(cuts) > 0:
        array = level_of(rng, dims, cuts, -0.22, 0.18) * array
    return jnp.clip(array, min=-most, max=most).astype(held_as)


def setup_inputs(seed: int = 0) -> dict:
    seeds = jax.random.split(jax.random.key(seed), 6)
    return {
        "observed": scatter_about(seeds[0], (STEPS, STATE, MEMBERS), 1.0, 6.0, ((0, 8), (1, 4)), jnp.float32),
        "gain": scatter_about(seeds[1], (N_SPACE, TILE, TILE), (10 * TILE) ** -0.5, 0.15625, ((0, 4),), jnp.float32),
        "trans": draw_trans(jax.random.fold_in(seeds[5], 71), 0),
        "dynamics": draw_dynamics(jax.random.fold_in(seeds[5], 71), 0),
        "smooth_gain": draw_smooth_gain(jax.random.fold_in(seeds[5], 71), 0),
    }


highest_mode = lax.Precision.HIGHEST


def apply_band(banded, current):
    count_tiles = banded.shape[0]
    tile_width = banded.shape[2]
    blocks = current.reshape(current.shape[0], count_tiles, tile_width, current.shape[2])
    empty_tile = jnp.zeros_like(blocks[:, :1])
    padded = jnp.concatenate([empty_tile, blocks, empty_tile], 1)
    stacked = jnp.concatenate([padded[:, :-2], padded[:, 1:-1], padded[:, 2:]], 2)
    result = jnp.einsum("crs,ncre->ncse", banded, stacked, precision=highest_mode)
    return result.reshape(current.shape)


def reference(observed, gain, trans, dynamics, smooth_gain):
    count_tiles = gain.shape[0]
    tile_width = gain.shape[1]
    steps = observed.shape[0]
    members = observed.shape[2]
    blocks = observed.reshape(steps, count_tiles, tile_width, members)
    forcing = jnp.einsum("cos,tcoe->tcse", gain, blocks, precision=highest_mode).reshape(observed.shape)

    def forward(carry, force):
        current = apply_band(trans, carry[None])[0] + force
        return current, current

    start = jnp.zeros(observed.shape[1:], jnp.float32)
    final_state, filtered = lax.scan(forward, start, forcing)
    mixed = apply_band(smooth_gain, apply_band(dynamics, filtered))
    innovation = jnp.concatenate([(filtered - mixed)[:-1], filtered[-1:]], 0)

    def backward(carry, drive):
        current = apply_band(smooth_gain, carry[None])[0] + drive
        return current, current

    first_state, smoothed = lax.scan(backward, start, innovation, reverse=True)
    return filtered, smoothed
```

```python
from functools import partial

import jax
import jax.numpy as jnp
from jax import lax
from jax.experimental import pallas as pl
from jax.experimental.pallas import tpu as pltpu
from jax.sharding import PartitionSpec as P

highest_mode = lax.Precision.HIGHEST


def shifted(shard, axis, by):
    devices = lax.axis_size(axis)
    pairs = [(i, i + by) for i in range(devices) if 0 <= i + by < devices]
    return lax.ppermute(shard, axis, pairs)


def apply_full(banded, current):
    count_tiles = banded.shape[0]
    tile_width = banded.shape[2]
    blocks = current.reshape(current.shape[0], count_tiles, tile_width, current.shape[2])
    empty_tile = jnp.zeros_like(blocks[:, :1])
    padded = jnp.concatenate([empty_tile, blocks, empty_tile], 1)
    stacked = jnp.concatenate([padded[:, :-2], padded[:, 1:-1], padded[:, 2:]], 2)
    result = jnp.einsum("crs,ncre->ncse", banded, stacked, precision=highest_mode)
    return result.reshape(current.shape)


def sweep(apply_step, inputs, entry, backward):
    length = inputs.shape[0]
    order = list(range(length - 1, -1, -1)) if backward else list(range(length))
    current = entry
    outputs = [entry] * length
    for moment in order:
        current = apply_step(current[None])[0] + inputs[moment]
        outputs[moment] = current
    return jnp.stack(outputs)


def carry_prefix(carry, tables, which, direction):
    total = carry
    for level in range(len(tables) + 1):
        reach = direction * (1 if level == 0 else 2 ** (level - 1))
        moved = shifted(total, "tm", reach)
        if level == 0:
            total = moved
        else:
            table = tables[level - 1][which]

            def term(start, count, table=table, moved=moved):
                return lax.dot_general(
                    table, moved, (((0,), (0,)), ((), ())), precision=highest_mode
                )

            total = total + lax.psum_scatter(
                term(jnp.int32(0), moved.shape[0] * lax.axis_size("space")),
                "space",
                scatter_dimension=0,
                tiled=True,
            )
    return total


def body(observed, gain, trans, dynamics, smooth_gain):
    steps, tile_width, members = observed.shape
    count_tiles = lax.axis_size("space")
    ranks = lax.axis_size("tm")
    place = lax.axis_index("tm")
    column = lax.axis_index("space")
    state_width = tile_width * count_tiles
    block_cols = state_width // ranks
    sections = (ranks - 1).bit_length()
    log_steps = steps.bit_length() - 1
    forcing = jnp.einsum("os,toe->tse", gain[0], observed, precision=highest_mode)
    full_trans, full_smooth, full_dynamics = (
        lax.all_gather(trans, "space", axis=0, tiled=True),
        lax.all_gather(smooth_gain, "space", axis=0, tiled=True),
        lax.all_gather(dynamics, "space", axis=0, tiled=True),
    )

    def first_block(full):
        target = place * block_cols // tile_width
        offset = place * block_cols % tile_width
        index = jnp.clip(target, 0, full.shape[0] - 1)
        slab = lax.dynamic_index_in_dim(full, index, 0, keepdims=False)
        row_start = jnp.clip(column - target + 1, 0, 2) * tile_width
        piece = lax.dynamic_slice(slab, (row_start, offset), (tile_width, block_cols))
        inside = (jnp.abs(column - target) <= 1).astype(jnp.float32)
        return piece * inside

    blocks = (first_block(full_trans), first_block(full_smooth))
    needed = []
    for level in range(log_steps + sections - 1):
        col_trans = lax.all_gather(blocks[0], "space", axis=0, tiled=True)
        col_smooth = lax.all_gather(blocks[1], "space", axis=0, tiled=True)
        blocks = (
            jnp.dot(
                lax.all_gather(blocks[0], "tm", axis=1, tiled=True),
                col_trans,
                precision=highest_mode,
            ),
            jnp.dot(
                lax.all_gather(blocks[1], "tm", axis=1, tiled=True),
                col_smooth,
                precision=highest_mode,
            ),
        )
        if level + 1 >= log_steps:
            needed.append(blocks)
    tables = []
    for pair in needed:
        tables.append(
            (
                lax.all_gather(pair[0], "tm", axis=1, tiled=True),
                lax.all_gather(pair[1], "tm", axis=1, tiled=True),
            )
        )
    final_moment = jnp.arange(steps)[:, None, None] == steps - 1
    at_end = jnp.logical_and(final_moment, place == ranks - 1)
    whole_forcing = lax.all_gather(forcing, "space", axis=1, tiled=True)
    zero_full = jnp.zeros((state_width, members), jnp.float32)
    step_trans = partial(apply_full, full_trans)
    step_smooth = partial(apply_full, full_smooth)
    trial = sweep(step_trans, whole_forcing, zero_full, False)
    own_tail = lax.dynamic_slice_in_dim(trial[steps - 1], column * tile_width, tile_width, 0)
    entry = carry_prefix(own_tail, tables, 0, 1)
    entry_full = lax.all_gather(entry, "space", axis=0, tiled=True)
    filtered_full = sweep(step_trans, whole_forcing, entry_full, False)
    mixed_full = apply_full(full_smooth, apply_full(full_dynamics, filtered_full))
    innovation_full = jnp.where(at_end, filtered_full, filtered_full - mixed_full)
    trial_back = sweep(step_smooth, innovation_full, zero_full, True)
    own_head = lax.dynamic_slice_in_dim(trial_back[0], column * tile_width, tile_width, 0)
    exit_state = carry_prefix(own_head, tables, 1, -1)
    exit_full = lax.all_gather(exit_state, "space", axis=0, tiled=True)
    smoothed_full = sweep(step_smooth, innovation_full, exit_full, True)
    filtered = lax.dynamic_slice_in_dim(filtered_full, column * tile_width, tile_width, 1)
    smoothed = lax.dynamic_slice_in_dim(smoothed_full, column * tile_width, tile_width, 1)
    return (filtered, smoothed)

MESH = pl.DeviceIdType.MESH
SUBLANES = 8


def pieces(x):
    high = x.astype(jnp.bfloat16)
    rest = x - high.astype(jnp.float32)
    mid = rest.astype(jnp.bfloat16)
    low = (rest - mid.astype(jnp.float32)).astype(jnp.bfloat16)
    return high, mid, low


def dot(a, b):
    return jnp.dot(a, b, preferred_element_type=jnp.float32)


def times(x, table):
    rows = x.shape[0]
    high = x.astype(jnp.bfloat16).astype(jnp.float32)
    both = jnp.concatenate([high, x - high], 0).astype(jnp.bfloat16)
    two = dot(both, table[0]) + dot(both, table[1])
    return two[:rows] + two[rows:] + dot(high.astype(jnp.bfloat16), table[2])


def square(table, result):
    width = table.shape[1]
    part = min(width, 256)

    def one(index, _):
        rows = pl.ds(pl.multiple_of(index * part, part), part)
        high, mid, low = table[0, rows, :], table[1, rows, :], table[2, rows, :]
        three = dot(jnp.concatenate([high, mid, low], 0), table[0])
        two = dot(jnp.concatenate([high, mid], 0), table[1])
        small = three[2 * part :] + two[part:] + dot(high, table[2])
        total = three[:part] + (two[:part] + three[part : 2 * part] + small)
        for place, piece in enumerate(pieces(total)):
            result[place, rows, :] = piece
        return 0

    lax.fori_loop(0, width // part, one, 0)


def swap_halves(x):
    return pltpu.roll(x, SUBLANES // 2, x.ndim - 2)


def upper_half(shape):
    return lax.broadcasted_iota(jnp.int32, shape, len(shape) - 2) < SUBLANES // 2


def interleave(first, second):
    upper = upper_half(first.shape)
    return (
        jnp.where(upper, first, swap_halves(second)),
        jnp.where(upper, swap_halves(first), second),
    )


def kernel(
    ranks, columns, observed, gain, trans, dynamics, smooth_gain, filtered, smoothed,
    outbox, forcing, states, drive, results, inbox_f, inbox_s, entries, summed, raw,
    trans_1, trans_p, trans_4, trans_8, smooth_1, smooth_4, smooth_8, dyn_1,
    table_send, table_recv, table_own, force_send, force_recv, filt_send, filt_recv, smoo_send, smoo_recv, own_sem,
):
    steps, tile_width, members = observed.shape
    devices = ranks * columns
    short = steps // 2
    state_width = columns * tile_width
    rank = lax.axis_index("tm")
    column = lax.axis_index("space")
    me = rank * columns + column
    beside = column + 1 - 2 * (column % 2)
    across = (column + 2) % columns

    barrier = pltpu.get_barrier_semaphore()

    def greet(offset, _):
        other = (me + offset) % devices
        pl.semaphore_signal(
            barrier, inc=1, device_id=(other // columns, other % columns), device_id_type=MESH
        )
        return 0

    lax.fori_loop(1, devices, greet, 0)

    sources = (trans, smooth_gain, dynamics)
    for which, source in enumerate(sources):
        pltpu.make_async_copy(source.at[0], raw.at[which, column], table_own.at[which]).start()

    groups = members // SUBLANES

    def force(step, _):
        halves = []
        for half in range(2):
            image = observed[half * short + step].T
            value = jnp.dot(image, gain[0], precision=highest_mode, preferred_element_type=jnp.float32)
            halves.append(value.reshape(groups, SUBLANES, tile_width))
        even, odd = interleave(*halves)
        outbox[:, 0, pl.ds(step, 1)] = even[:, None]
        outbox[:, 1, pl.ds(step, 1)] = odd[:, None]
        return 0

    lax.fori_loop(0, short, force, 0)
    pl.semaphore_wait(barrier, devices - 1)

    def table_copy(which, what, source_column, target):
        return pltpu.make_async_remote_copy(
            src_ref=sources[which].at[0] if what < 2 else raw.at[which, source_column],
            dst_ref=raw.at[which, source_column],
            send_sem=table_send.at[which, what],
            recv_sem=table_recv.at[which, what],
            device_id=(rank, target),
            device_id_type=MESH,
        )

    def send_table(which):
        table_copy(which, 0, column, across).start()
        table_copy(which, 1, column, beside).start()

    def relay_table(which):
        table_copy(which, 0, column, across).wait_recv()
        table_copy(which, 2, across, beside).start()

    def finish_table(which):
        pltpu.make_async_copy(sources[which].at[0], raw.at[which, column], table_own.at[which]).wait()
        table_copy(which, 1, column, beside).wait_recv()
        table_copy(which, 2, across, beside).wait_recv()

    def build(which, table):
        for tile in range(columns):
            lanes = slice(tile * tile_width, (tile + 1) * tile_width)
            for row in range(columns):
                rows = slice(row * tile_width, (row + 1) * tile_width)
                shift = row - tile + 1
                if 0 <= shift <= 2:
                    block = raw[which, tile, shift * tile_width : (shift + 1) * tile_width, :]
                    for place, piece in enumerate(pieces(block)):
                        table[place, rows, lanes] = piece
                else:
                    for place in range(3):
                        table[place, rows, lanes] = jnp.zeros((tile_width, tile_width), jnp.bfloat16)

    def lane_part(index):
        return pl.ds(pl.multiple_of(index * tile_width, tile_width), tile_width)

    def force_copy(offset):
        other = (me + offset) % devices
        return pltpu.make_async_remote_copy(
            src_ref=outbox.at[other // 2, other % 2],
            dst_ref=forcing.at[:, rank, :, lane_part(column)],
            send_sem=force_send.at[offset],
            recv_sem=force_recv.at[offset],
            device_id=(other // columns, other % columns),
            device_id_type=MESH,
        )

    def result_copy(offset, source, inbox, send, recv):
        other = (me + offset) % devices
        return pltpu.make_async_remote_copy(
            src_ref=source.at[:, other // columns, :, lane_part(other % columns)],
            dst_ref=inbox.at[me // 2, me % 2],
            send_sem=send.at[offset],
            recv_sem=recv.at[offset],
            device_id=(other // columns, other % columns),
            device_id_type=MESH,
        )

    def over_others(act):
        def one(offset, _):
            act(offset)
            return 0

        lax.fori_loop(1, devices, one, 0)

    send_table(0)
    over_others(lambda offset: force_copy(offset).start())
    own_force = pltpu.make_async_copy(
        outbox.at[me // 2, me % 2], forcing.at[:, rank, :, lane_part(column)], own_sem.at[0]
    )
    own_force.start()
    send_table(1)
    send_table(2)

    relay_table(0)
    finish_table(0)
    build(0, trans_1)
    square(trans_1, trans_p)
    square(trans_p, trans_4)
    relay_table(1)
    relay_table(2)
    square(trans_4, trans_8)
    finish_table(1)
    build(1, smooth_1)
    square(smooth_1, trans_p)
    square(trans_p, smooth_4)
    square(smooth_4, smooth_8)
    finish_table(2)
    build(2, dyn_1)

    over_others(lambda offset: force_copy(offset).wait_recv())
    own_force.wait()

    rows = ranks * SUBLANES
    whole = (ranks, SUBLANES, state_width)

    def flat(x):
        return x.reshape(rows, state_width)

    def trial(inputs, order, table):
        def one(index, current):
            return times(current, table) + flat(inputs[order(index)])

        return lax.fori_loop(1, short, one, flat(inputs[order(0)]))

    def chain(order, table):
        entries[order(0)] = jnp.zeros((SUBLANES, state_width), jnp.float32)
        entries[order(1)] = summed[order(0)]

        def one(index, current):
            current = times(current, table) + summed[order(index)]
            entries[order(index + 1)] = current
            return current

        lax.fori_loop(1, ranks - 1, one, summed[order(0)])

    def final(inputs, order, table, entry, outputs):
        def one(index, current):
            current = times(current, table) + flat(inputs[order(index)])
            outputs[order(index)] = current.reshape(whole)
            return current

        lax.fori_loop(0, short, one, entry)

    forward = lambda index: index
    upper = upper_half(whole)
    ends = trial(forcing, forward, trans_1)
    halves = ends.reshape(whole)
    summed[...] = times(ends, trans_4).reshape(whole) + swap_halves(halves)
    chain(forward, trans_8)
    first = entries[...]
    second = times(flat(first), trans_4).reshape(whole) + halves
    final(forcing, forward, trans_1, flat(jnp.where(upper, first, swap_halves(second))), states)

    over_others(lambda offset: result_copy(offset, states, inbox_f, filt_send, filt_recv).start())
    own_filtered = pltpu.make_async_copy(
        states.at[:, rank, :, lane_part(column)], inbox_f.at[me // 2, me % 2], own_sem.at[1]
    )
    own_filtered.start()

    def innovate(step, _):
        value = flat(states[step])
        mixed = times(times(value, dyn_1), smooth_1)
        place = lax.broadcasted_iota(jnp.int32, mixed.shape, 0)
        at_end = jnp.logical_and(place >= rows - SUBLANES // 2, step == short - 1)
        drive[step] = jnp.where(at_end, value, value - mixed).reshape(whole)
        return 0

    lax.fori_loop(0, short, innovate, 0)

    backward = lambda index: short - 1 - index
    heads = trial(drive, backward, smooth_1)
    halves = heads.reshape(whole)
    summed[...] = swap_halves(times(heads, smooth_4).reshape(whole)) + halves
    chain(lambda index: ranks - 1 - index, smooth_8)
    last = entries[...]
    before = times(flat(last), smooth_4).reshape(whole) + swap_halves(halves)
    final(drive, backward, smooth_1, flat(jnp.where(upper, before, swap_halves(last))), results)

    over_others(lambda offset: result_copy(offset, results, inbox_s, smoo_send, smoo_recv).start())
    own_smoothed = pltpu.make_async_copy(
        results.at[:, rank, :, lane_part(column)], inbox_s.at[me // 2, me % 2], own_sem.at[2]
    )
    own_smoothed.start()

    def deliver(inbox, output):
        def one(step, _):
            parts = interleave(inbox[:, 0, step], inbox[:, 1, step])
            for half, part in enumerate(parts):
                output[half * short + step] = part.reshape(members, tile_width).T
            return 0

        lax.fori_loop(0, short, one, 0)

    over_others(lambda offset: result_copy(offset, states, inbox_f, filt_send, filt_recv).wait_recv())
    own_filtered.wait()
    deliver(inbox_f, filtered)
    over_others(lambda offset: result_copy(offset, results, inbox_s, smoo_send, smoo_recv).wait_recv())
    own_smoothed.wait()
    deliver(inbox_s, smoothed)

    for which in range(3):
        table_copy(which, 0, column, across).wait_send()
        table_copy(which, 1, column, beside).wait_send()
        table_copy(which, 2, across, beside).wait_send()
    over_others(lambda offset: force_copy(offset).wait_send())
    over_others(lambda offset: result_copy(offset, states, inbox_f, filt_send, filt_recv).wait_send())
    over_others(lambda offset: result_copy(offset, results, inbox_s, smoo_send, smoo_recv).wait_send())


def member_body(ranks, columns, observed, gain, trans, dynamics, smooth_gain):
    steps, tile_width, members = observed.shape
    devices = ranks * columns
    short = steps // 2
    width = columns * tile_width
    pairs = devices // 2
    boxes = pltpu.VMEM((pairs, 2, short, SUBLANES, tile_width), jnp.float32)
    series = pltpu.VMEM((short, ranks, SUBLANES, width), jnp.float32)
    block = pltpu.VMEM((ranks, SUBLANES, width), jnp.float32)
    table = pltpu.VMEM((3, width, width), jnp.bfloat16)
    each = pltpu.SemaphoreType.DMA((devices,))
    vmem = pl.BlockSpec(memory_space=pltpu.VMEM)
    return pl.pallas_call(
        partial(kernel, ranks, columns),
        out_shape=[jax.ShapeDtypeStruct(observed.shape, jnp.float32)] * 2,
        in_specs=[vmem] * 5,
        out_specs=[vmem] * 2,
        scratch_shapes=[
            boxes, series, series, series, series, boxes, boxes, block, block,
            pltpu.VMEM((3, columns, 3 * tile_width, tile_width), jnp.float32),
            table, table, table, table, table, table, table, table,
            pltpu.SemaphoreType.DMA((3, 3)),
            pltpu.SemaphoreType.DMA((3, 3)),
            pltpu.SemaphoreType.DMA((3,)),
            each, each, each, each, each, each,
            pltpu.SemaphoreType.DMA((3,)),
        ],
        compiler_params=pltpu.CompilerParams(
            collective_id=0, has_side_effects=True, vmem_limit_bytes=56 * 2**20
        ),
    )(observed, gain, trans, dynamics, smooth_gain)


def by_members(mesh, observed, gain, trans, dynamics, smooth_gain):
    ranks, columns = mesh.shape["tm"], mesh.shape["space"]
    devices = ranks * columns
    steps, tile_width, members = observed.shape
    fits = (
        members * 2 == devices * SUBLANES
        and steps % 2 == 0
        and columns == 4
        and ranks >= 3
        and tile_width == 128
        and members == 128
    )
    if fits:
        return tuple(member_body(ranks, columns, observed, gain, trans, dynamics, smooth_gain))
    return body(observed, gain, trans, dynamics, smooth_gain)


def solution(mesh):
    return jax.shard_map(
        partial(by_members, mesh),
        mesh=mesh,
        in_specs=(
            P("tm", "space", None),
            P("space", None, None),
            P("space", None, None),
            P("space", None, None),
            P("space", None, None),
        ),
        out_specs=(P("tm", "space", None), P("tm", "space", None)),
        check_vma=False,
    )
```

```python
from functools import partial

import jax
import jax.numpy as jnp
from jax import lax
from jax.experimental import pallas as pl
from jax.experimental.pallas import tpu as pltpu
from jax.sharding import PartitionSpec as P

highest_mode = lax.Precision.HIGHEST


def shifted(shard, axis, by):
    devices = lax.axis_size(axis)
    pairs = [(i, i + by) for i in range(devices) if 0 <= i + by < devices]
    return lax.ppermute(shard, axis, pairs)


def apply_full(banded, current):
    count_tiles = banded.shape[0]
    tile_width = banded.shape[2]
    blocks = current.reshape(current.shape[0], count_tiles, tile_width, current.shape[2])
    empty_tile = jnp.zeros_like(blocks[:, :1])
    padded = jnp.concatenate([empty_tile, blocks, empty_tile], 1)
    stacked = jnp.concatenate([padded[:, :-2], padded[:, 1:-1], padded[:, 2:]], 2)
    result = jnp.einsum("crs,ncre->ncse", banded, stacked, precision=highest_mode)
    return result.reshape(current.shape)


def sweep(apply_step, inputs, entry, backward):
    length = inputs.shape[0]
    order = list(range(length - 1, -1, -1)) if backward else list(range(length))
    current = entry
    outputs = [entry] * length
    for moment in order:
        current = apply_step(current[None])[0] + inputs[moment]
        outputs[moment] = current
    return jnp.stack(outputs)


def carry_prefix(carry, tables, which, direction):
    total = carry
    for level in range(len(tables) + 1):
        reach = direction * (1 if level == 0 else 2 ** (level - 1))
        moved = shifted(total, "tm", reach)
        if level == 0:
            total = moved
        else:
            table = tables[level - 1][which]

            def term(start, count, table=table, moved=moved):
                return lax.dot_general(
                    table, moved, (((0,), (0,)), ((), ())), precision=highest_mode
                )

            total = total + lax.psum_scatter(
                term(jnp.int32(0), moved.shape[0] * lax.axis_size("space")),
                "space",
                scatter_dimension=0,
                tiled=True,
            )
    return total


def body(observed, gain, trans, dynamics, smooth_gain):
    steps, tile_width, members = observed.shape
    count_tiles = lax.axis_size("space")
    ranks = lax.axis_size("tm")
    place = lax.axis_index("tm")
    column = lax.axis_index("space")
    state_width = tile_width * count_tiles
    block_cols = state_width // ranks
    sections = (ranks - 1).bit_length()
    log_steps = steps.bit_length() - 1
    forcing = jnp.einsum("os,toe->tse", gain[0], observed, precision=highest_mode)
    full_trans, full_smooth, full_dynamics = (
        lax.all_gather(trans, "space", axis=0, tiled=True),
        lax.all_gather(smooth_gain, "space", axis=0, tiled=True),
        lax.all_gather(dynamics, "space", axis=0, tiled=True),
    )

    def first_block(full):
        target = place * block_cols // tile_width
        offset = place * block_cols % tile_width
        index = jnp.clip(target, 0, full.shape[0] - 1)
        slab = lax.dynamic_index_in_dim(full, index, 0, keepdims=False)
        row_start = jnp.clip(column - target + 1, 0, 2) * tile_width
        piece = lax.dynamic_slice(slab, (row_start, offset), (tile_width, block_cols))
        inside = (jnp.abs(column - target) <= 1).astype(jnp.float32)
        return piece * inside

    blocks = (first_block(full_trans), first_block(full_smooth))
    needed = []
    for level in range(log_steps + sections - 1):
        col_trans = lax.all_gather(blocks[0], "space", axis=0, tiled=True)
        col_smooth = lax.all_gather(blocks[1], "space", axis=0, tiled=True)
        blocks = (
            jnp.dot(
                lax.all_gather(blocks[0], "tm", axis=1, tiled=True),
                col_trans,
                precision=highest_mode,
            ),
            jnp.dot(
                lax.all_gather(blocks[1], "tm", axis=1, tiled=True),
                col_smooth,
                precision=highest_mode,
            ),
        )
        if level + 1 >= log_steps:
            needed.append(blocks)
    tables = []
    for pair in needed:
        tables.append(
            (
                lax.all_gather(pair[0], "tm", axis=1, tiled=True),
                lax.all_gather(pair[1], "tm", axis=1, tiled=True),
            )
        )
    final_moment = jnp.arange(steps)[:, None, None] == steps - 1
    at_end = jnp.logical_and(final_moment, place == ranks - 1)
    whole_forcing = lax.all_gather(forcing, "space", axis=1, tiled=True)
    zero_full = jnp.zeros((state_width, members), jnp.float32)
    step_trans = partial(apply_full, full_trans)
    step_smooth = partial(apply_full, full_smooth)
    trial = sweep(step_trans, whole_forcing, zero_full, False)
    own_tail = lax.dynamic_slice_in_dim(trial[steps - 1], column * tile_width, tile_width, 0)
    entry = carry_prefix(own_tail, tables, 0, 1)
    entry_full = lax.all_gather(entry, "space", axis=0, tiled=True)
    filtered_full = sweep(step_trans, whole_forcing, entry_full, False)
    mixed_full = apply_full(full_smooth, apply_full(full_dynamics, filtered_full))
    innovation_full = jnp.where(at_end, filtered_full, filtered_full - mixed_full)
    trial_back = sweep(step_smooth, innovation_full, zero_full, True)
    own_head = lax.dynamic_slice_in_dim(trial_back[0], column * tile_width, tile_width, 0)
    exit_state = carry_prefix(own_head, tables, 1, -1)
    exit_full = lax.all_gather(exit_state, "space", axis=0, tiled=True)
    smoothed_full = sweep(step_smooth, innovation_full, exit_full, True)
    filtered = lax.dynamic_slice_in_dim(filtered_full, column * tile_width, tile_width, 1)
    smoothed = lax.dynamic_slice_in_dim(smoothed_full, column * tile_width, tile_width, 1)
    return (filtered, smoothed)

MESH = pl.DeviceIdType.MESH
SUBLANES = 8
SPLIT = (1, 2)


def pieces(x):
    high = x.astype(jnp.bfloat16)
    return high, (x - high.astype(jnp.float32)).astype(jnp.bfloat16)


def dot(a, b):
    return jnp.dot(a, b, preferred_element_type=jnp.float32)


def times(x, table):
    rows = x.shape[0]
    high = x.astype(jnp.bfloat16).astype(jnp.float32)
    both = jnp.concatenate([high, x - high], 0).astype(jnp.bfloat16)
    two = dot(both, table[0]) + dot(both, table[1])
    return two[:rows] + two[rows:]


def square(table, result):
    width = table.shape[1]
    part = min(width, 256)

    def one(index, _):
        rows = pl.ds(pl.multiple_of(index * part, part), part)
        high, low = table[0, rows, :], table[1, rows, :]
        two = dot(jnp.concatenate([high, low], 0), table[0])
        total = two[:part] + (two[part:] + dot(high, table[1]))
        for place, piece in enumerate(pieces(total)):
            result[place, rows, :] = piece
        return 0

    lax.fori_loop(0, width // part, one, 0)


def swap_halves(x):
    return pltpu.roll(x, SUBLANES // 2, x.ndim - 2)


def upper_half(shape):
    return lax.broadcasted_iota(jnp.int32, shape, len(shape) - 2) < SUBLANES // 2


def interleave(first, second):
    upper = upper_half(first.shape)
    return (
        jnp.where(upper, first, swap_halves(second)),
        jnp.where(upper, swap_halves(first), second),
    )


def kernel(
    ranks, columns, observed, gain, trans, dynamics, smooth_gain, filtered, smoothed,
    outbox, forcing, states, drive, results, inbox_f, inbox_s, entries, summed, raw,
    trans_1, trans_p, trans_4, trans_8, smooth_1, smooth_4, smooth_8, dyn_1,
    table_send, table_recv, table_own, force_send, force_recv, filt_send, filt_recv, smoo_send, smoo_recv, own_sem,
):
    steps, tile_width, members = observed.shape
    devices = ranks * columns
    short = steps // 2
    state_width = columns * tile_width
    rank = lax.axis_index("tm")
    column = lax.axis_index("space")
    me = rank * columns + column
    beside = column + 1 - 2 * (column % 2)
    across = (column + 2) % columns

    barrier = pltpu.get_barrier_semaphore()

    def greet(offset, _):
        other = (me + offset) % devices
        pl.semaphore_signal(
            barrier, inc=1, device_id=(other // columns, other % columns), device_id_type=MESH
        )
        return 0

    lax.fori_loop(1, devices, greet, 0)

    sources = (trans, smooth_gain, dynamics)
    for which, source in enumerate(sources):
        pltpu.make_async_copy(source.at[0], raw.at[which, column], table_own.at[which]).start()

    groups = members // SUBLANES

    def force(step, _):
        halves = []
        for half in range(2):
            image = observed[half * short + step].T
            value = jnp.dot(image, gain[0], precision=highest_mode, preferred_element_type=jnp.float32)
            halves.append(value.reshape(groups, SUBLANES, tile_width))
        even, odd = interleave(*halves)
        outbox[:, 0, pl.ds(step, 1)] = even[:, None]
        outbox[:, 1, pl.ds(step, 1)] = odd[:, None]
        return 0

    lax.fori_loop(0, short, force, 0)
    pl.semaphore_wait(barrier, devices - 1)

    shared = rank % 2
    partner = rank + 1 - 2 * shared

    def half_rows(index):
        count = 3 * tile_width // 2
        return pl.ds(pl.multiple_of(index * count, count), count)

    def table_copy(which, what):
        split = which in SPLIT
        if what == 0:
            place, to = column, (rank, across)
            rows = half_rows(shared) if split else slice(None)
        elif what == 1:
            place, to, rows = column, (rank, beside), slice(None)
        elif what == 2:
            place, to = across, (rank, beside)
            rows = half_rows(shared) if split else slice(None)
        elif what == 3:
            place, to, rows = across, (partner, column), half_rows(shared)
        else:
            place, to, rows = across, (rank, beside), half_rows(1 - shared)
        source = sources[which].at[0, rows] if what < 2 else raw.at[which, place, rows]
        return pltpu.make_async_remote_copy(
            src_ref=source,
            dst_ref=raw.at[which, place, rows],
            send_sem=table_send.at[which, what],
            recv_sem=table_recv.at[which, what],
            device_id=to,
            device_id_type=MESH,
        )

    def send_table(which):
        table_copy(which, 0).start()
        table_copy(which, 1).start()

    def relay_table(which):
        table_copy(which, 0).wait_recv()
        table_copy(which, 2).start()
        if which in SPLIT:
            table_copy(which, 3).start()

    def relay_again(which):
        if which in SPLIT:
            table_copy(which, 3).wait_recv()
            table_copy(which, 4).start()

    def finish_table(which):
        pltpu.make_async_copy(sources[which].at[0], raw.at[which, column], table_own.at[which]).wait()
        table_copy(which, 1).wait_recv()
        table_copy(which, 2).wait_recv()
        if which in SPLIT:
            table_copy(which, 4).wait_recv()

    def build(which, table):
        for tile in range(columns):
            lanes = slice(tile * tile_width, (tile + 1) * tile_width)
            for row in range(columns):
                rows = slice(row * tile_width, (row + 1) * tile_width)
                shift = row - tile + 1
                if 0 <= shift <= 2:
                    block = raw[which, tile, shift * tile_width : (shift + 1) * tile_width, :]
                    for place, piece in enumerate(pieces(block)):
                        table[place, rows, lanes] = piece
                else:
                    for place in range(2):
                        table[place, rows, lanes] = jnp.zeros((tile_width, tile_width), jnp.bfloat16)

    def lane_part(index):
        return pl.ds(pl.multiple_of(index * tile_width, tile_width), tile_width)

    def force_copy(offset):
        other = (me + offset) % devices
        return pltpu.make_async_remote_copy(
            src_ref=outbox.at[other // 2, other % 2],
            dst_ref=forcing.at[:, rank, :, lane_part(column)],
            send_sem=force_send.at[offset],
            recv_sem=force_recv.at[offset],
            device_id=(other // columns, other % columns),
            device_id_type=MESH,
        )

    def result_copy(offset, source, inbox, send, recv):
        other = (me + offset) % devices
        return pltpu.make_async_remote_copy(
            src_ref=source.at[:, other // columns, :, lane_part(other % columns)],
            dst_ref=inbox.at[me // 2, me % 2],
            send_sem=send.at[offset],
            recv_sem=recv.at[offset],
            device_id=(other // columns, other % columns),
            device_id_type=MESH,
        )

    def over_others(act):
        def one(offset, _):
            act(offset)
            return 0

        lax.fori_loop(1, devices, one, 0)

    send_table(0)
    over_others(lambda offset: force_copy(offset).start())
    own_force = pltpu.make_async_copy(
        outbox.at[me // 2, me % 2], forcing.at[:, rank, :, lane_part(column)], own_sem.at[0]
    )
    own_force.start()
    send_table(1)
    send_table(2)

    relay_table(0)
    finish_table(0)
    build(0, trans_1)
    square(trans_1, trans_p)
    square(trans_p, trans_4)
    square(trans_4, trans_8)
    over_others(lambda offset: force_copy(offset).wait_recv())
    own_force.wait()

    relay_table(1)
    rows = ranks * SUBLANES
    whole = (ranks, SUBLANES, state_width)

    def flat(x):
        return x.reshape(rows, state_width)

    def trial(inputs, order, table):
        def one(index, current):
            return times(current, table) + flat(inputs[order(index)])

        return lax.fori_loop(1, short, one, flat(inputs[order(0)]))

    def chain(order, table):
        entries[order(0)] = jnp.zeros((SUBLANES, state_width), jnp.float32)
        entries[order(1)] = summed[order(0)]

        def one(index, current):
            current = times(current, table) + summed[order(index)]
            entries[order(index + 1)] = current
            return current

        lax.fori_loop(1, ranks - 1, one, summed[order(0)])

    def final(inputs, order, table, entry, outputs):
        def one(index, current):
            current = times(current, table) + flat(inputs[order(index)])
            outputs[order(index)] = current.reshape(whole)
            return current

        lax.fori_loop(0, short, one, entry)

    forward = lambda index: index
    upper = upper_half(whole)
    ends = trial(forcing, forward, trans_1)
    halves = ends.reshape(whole)
    summed[...] = times(ends, trans_4).reshape(whole) + swap_halves(halves)
    relay_table(2)
    relay_again(1)
    chain(forward, trans_8)
    first = entries[...]
    second = times(flat(first), trans_4).reshape(whole) + halves
    relay_again(2)
    final(forcing, forward, trans_1, flat(jnp.where(upper, first, swap_halves(second))), states)

    over_others(lambda offset: result_copy(offset, states, inbox_f, filt_send, filt_recv).start())
    own_filtered = pltpu.make_async_copy(
        states.at[:, rank, :, lane_part(column)], inbox_f.at[me // 2, me % 2], own_sem.at[1]
    )
    own_filtered.start()

    finish_table(1)
    build(1, smooth_1)
    square(smooth_1, trans_p)
    square(trans_p, smooth_4)
    square(smooth_4, smooth_8)
    finish_table(2)
    build(2, dyn_1)

    def innovate(step, _):
        value = flat(states[step])
        mixed = times(times(value, dyn_1), smooth_1)
        place = lax.broadcasted_iota(jnp.int32, mixed.shape, 0)
        at_end = jnp.logical_and(place >= rows - SUBLANES // 2, step == short - 1)
        drive[step] = jnp.where(at_end, value, value - mixed).reshape(whole)
        return 0

    lax.fori_loop(0, short, innovate, 0)

    backward = lambda index: short - 1 - index
    heads = trial(drive, backward, smooth_1)
    halves = heads.reshape(whole)
    summed[...] = swap_halves(times(heads, smooth_4).reshape(whole)) + halves
    chain(lambda index: ranks - 1 - index, smooth_8)
    last = entries[...]
    before = times(flat(last), smooth_4).reshape(whole) + swap_halves(halves)
    final(drive, backward, smooth_1, flat(jnp.where(upper, before, swap_halves(last))), results)

    over_others(lambda offset: result_copy(offset, results, inbox_s, smoo_send, smoo_recv).start())
    own_smoothed = pltpu.make_async_copy(
        results.at[:, rank, :, lane_part(column)], inbox_s.at[me // 2, me % 2], own_sem.at[2]
    )
    own_smoothed.start()

    def deliver(inbox, output):
        def one(step, _):
            parts = interleave(inbox[:, 0, step], inbox[:, 1, step])
            for half, part in enumerate(parts):
                output[half * short + step] = part.reshape(members, tile_width).T
            return 0

        lax.fori_loop(0, short, one, 0)

    over_others(lambda offset: result_copy(offset, states, inbox_f, filt_send, filt_recv).wait_recv())
    own_filtered.wait()
    deliver(inbox_f, filtered)
    over_others(lambda offset: result_copy(offset, results, inbox_s, smoo_send, smoo_recv).wait_recv())
    own_smoothed.wait()
    deliver(inbox_s, smoothed)

    for which in range(3):
        for what in range(5 if which in SPLIT else 3):
            table_copy(which, what).wait_send()
    over_others(lambda offset: force_copy(offset).wait_send())
    over_others(lambda offset: result_copy(offset, states, inbox_f, filt_send, filt_recv).wait_send())
    over_others(lambda offset: result_copy(offset, results, inbox_s, smoo_send, smoo_recv).wait_send())


def member_body(ranks, columns, observed, gain, trans, dynamics, smooth_gain):
    steps, tile_width, members = observed.shape
    devices = ranks * columns
    short = steps // 2
    width = columns * tile_width
    pairs = devices // 2
    boxes = pltpu.VMEM((pairs, 2, short, SUBLANES, tile_width), jnp.float32)
    series = pltpu.VMEM((short, ranks, SUBLANES, width), jnp.float32)
    block = pltpu.VMEM((ranks, SUBLANES, width), jnp.float32)
    table = pltpu.VMEM((2, width, width), jnp.bfloat16)
    each = pltpu.SemaphoreType.DMA((devices,))
    vmem = pl.BlockSpec(memory_space=pltpu.VMEM)
    return pl.pallas_call(
        partial(kernel, ranks, columns),
        out_shape=[jax.ShapeDtypeStruct(observed.shape, jnp.float32)] * 2,
        in_specs=[vmem] * 5,
        out_specs=[vmem] * 2,
        scratch_shapes=[
            boxes, series, series, series, series, boxes, boxes, block, block,
            pltpu.VMEM((3, columns, 3 * tile_width, tile_width), jnp.float32),
            table, table, table, table, table, table, table, table,
            pltpu.SemaphoreType.DMA((3, 5)),
            pltpu.SemaphoreType.DMA((3, 5)),
            pltpu.SemaphoreType.DMA((3,)),
            each, each, each, each, each, each,
            pltpu.SemaphoreType.DMA((3,)),
        ],
        compiler_params=pltpu.CompilerParams(
            collective_id=0, has_side_effects=True, vmem_limit_bytes=56 * 2**20
        ),
    )(observed, gain, trans, dynamics, smooth_gain)


def by_members(mesh, observed, gain, trans, dynamics, smooth_gain):
    ranks, columns = mesh.shape["tm"], mesh.shape["space"]
    devices = ranks * columns
    steps, tile_width, members = observed.shape
    fits = (
        members * 2 == devices * SUBLANES
        and steps % 2 == 0
        and columns == 4
        and ranks >= 3
        and tile_width == 128
        and members == 128
    )
    if fits:
        return tuple(member_body(ranks, columns, observed, gain, trans, dynamics, smooth_gain))
    return body(observed, gain, trans, dynamics, smooth_gain)


def solution(mesh):
    return jax.shard_map(
        partial(by_members, mesh),
        mesh=mesh,
        in_specs=(
            P("tm", "space", None),
            P("space", None, None),
            P("space", None, None),
            P("space", None, None),
            P("space", None, None),
        ),
        out_specs=(P("tm", "space", None), P("tm", "space", None)),
        check_vma=False,
    )
```

```python
from functools import partial

import jax
import jax.numpy as jnp
from jax import lax
from jax.experimental import pallas as pl
from jax.experimental.pallas import tpu as pltpu
from jax.sharding import PartitionSpec as P

highest_mode = lax.Precision.HIGHEST


def shifted(shard, axis, by):
    devices = lax.axis_size(axis)
    pairs = [(i, i + by) for i in range(devices) if 0 <= i + by < devices]
    return lax.ppermute(shard, axis, pairs)


def apply_full(banded, current):
    count_tiles = banded.shape[0]
    tile_width = banded.shape[2]
    blocks = current.reshape(current.shape[0], count_tiles, tile_width, current.shape[2])
    empty_tile = jnp.zeros_like(blocks[:, :1])
    padded = jnp.concatenate([empty_tile, blocks, empty_tile], 1)
    stacked = jnp.concatenate([padded[:, :-2], padded[:, 1:-1], padded[:, 2:]], 2)
    result = jnp.einsum("crs,ncre->ncse", banded, stacked, precision=highest_mode)
    return result.reshape(current.shape)


def sweep(apply_step, inputs, entry, backward):
    length = inputs.shape[0]
    order = list(range(length - 1, -1, -1)) if backward else list(range(length))
    current = entry
    outputs = [entry] * length
    for moment in order:
        current = apply_step(current[None])[0] + inputs[moment]
        outputs[moment] = current
    return jnp.stack(outputs)


def carry_prefix(carry, tables, which, direction):
    total = carry
    for level in range(len(tables) + 1):
        reach = direction * (1 if level == 0 else 2 ** (level - 1))
        moved = shifted(total, "tm", reach)
        if level == 0:
            total = moved
        else:
            table = tables[level - 1][which]

            def term(start, count, table=table, moved=moved):
                return lax.dot_general(
                    table, moved, (((0,), (0,)), ((), ())), precision=highest_mode
                )

            total = total + lax.psum_scatter(
                term(jnp.int32(0), moved.shape[0] * lax.axis_size("space")),
                "space",
                scatter_dimension=0,
                tiled=True,
            )
    return total


def body(observed, gain, trans, dynamics, smooth_gain):
    steps, tile_width, members = observed.shape
    count_tiles = lax.axis_size("space")
    ranks = lax.axis_size("tm")
    place = lax.axis_index("tm")
    column = lax.axis_index("space")
    state_width = tile_width * count_tiles
    block_cols = state_width // ranks
    sections = (ranks - 1).bit_length()
    log_steps = steps.bit_length() - 1
    forcing = jnp.einsum("os,toe->tse", gain[0], observed, precision=highest_mode)
    full_trans, full_smooth, full_dynamics = (
        lax.all_gather(trans, "space", axis=0, tiled=True),
        lax.all_gather(smooth_gain, "space", axis=0, tiled=True),
        lax.all_gather(dynamics, "space", axis=0, tiled=True),
    )

    def first_block(full):
        target = place * block_cols // tile_width
        offset = place * block_cols % tile_width
        index = jnp.clip(target, 0, full.shape[0] - 1)
        slab = lax.dynamic_index_in_dim(full, index, 0, keepdims=False)
        row_start = jnp.clip(column - target + 1, 0, 2) * tile_width
        piece = lax.dynamic_slice(slab, (row_start, offset), (tile_width, block_cols))
        inside = (jnp.abs(column - target) <= 1).astype(jnp.float32)
        return piece * inside

    blocks = (first_block(full_trans), first_block(full_smooth))
    needed = []
    for level in range(log_steps + sections - 1):
        col_trans = lax.all_gather(blocks[0], "space", axis=0, tiled=True)
        col_smooth = lax.all_gather(blocks[1], "space", axis=0, tiled=True)
        blocks = (
            jnp.dot(
                lax.all_gather(blocks[0], "tm", axis=1, tiled=True),
                col_trans,
                precision=highest_mode,
            ),
            jnp.dot(
                lax.all_gather(blocks[1], "tm", axis=1, tiled=True),
                col_smooth,
                precision=highest_mode,
            ),
        )
        if level + 1 >= log_steps:
            needed.append(blocks)
    tables = []
    for pair in needed:
        tables.append(
            (
                lax.all_gather(pair[0], "tm", axis=1, tiled=True),
                lax.all_gather(pair[1], "tm", axis=1, tiled=True),
            )
        )
    final_moment = jnp.arange(steps)[:, None, None] == steps - 1
    at_end = jnp.logical_and(final_moment, place == ranks - 1)
    whole_forcing = lax.all_gather(forcing, "space", axis=1, tiled=True)
    zero_full = jnp.zeros((state_width, members), jnp.float32)
    step_trans = partial(apply_full, full_trans)
    step_smooth = partial(apply_full, full_smooth)
    trial = sweep(step_trans, whole_forcing, zero_full, False)
    own_tail = lax.dynamic_slice_in_dim(trial[steps - 1], column * tile_width, tile_width, 0)
    entry = carry_prefix(own_tail, tables, 0, 1)
    entry_full = lax.all_gather(entry, "space", axis=0, tiled=True)
    filtered_full = sweep(step_trans, whole_forcing, entry_full, False)
    mixed_full = apply_full(full_smooth, apply_full(full_dynamics, filtered_full))
    innovation_full = jnp.where(at_end, filtered_full, filtered_full - mixed_full)
    trial_back = sweep(step_smooth, innovation_full, zero_full, True)
    own_head = lax.dynamic_slice_in_dim(trial_back[0], column * tile_width, tile_width, 0)
    exit_state = carry_prefix(own_head, tables, 1, -1)
    exit_full = lax.all_gather(exit_state, "space", axis=0, tiled=True)
    smoothed_full = sweep(step_smooth, innovation_full, exit_full, True)
    filtered = lax.dynamic_slice_in_dim(filtered_full, column * tile_width, tile_width, 1)
    smoothed = lax.dynamic_slice_in_dim(smoothed_full, column * tile_width, tile_width, 1)
    return (filtered, smoothed)

MESH = pl.DeviceIdType.MESH
SUBLANES = 8
SPLIT = (1, 2)


def pieces(x):
    high = x.astype(jnp.bfloat16)
    return high, (x - high.astype(jnp.float32)).astype(jnp.bfloat16)


def dot(a, b):
    return jnp.dot(a, b, preferred_element_type=jnp.float32)


def times(x, table):
    rows = x.shape[0]
    high = x.astype(jnp.bfloat16).astype(jnp.float32)
    both = jnp.concatenate([high, x - high], 0).astype(jnp.bfloat16)
    two = dot(both, table[0]) + dot(both, table[1])
    return two[:rows] + two[rows:]


def square(table, result):
    width = table.shape[1]
    part = min(width, 256)

    def one(index, _):
        rows = pl.ds(pl.multiple_of(index * part, part), part)
        high, low = table[0, rows, :], table[1, rows, :]
        two = dot(jnp.concatenate([high, low], 0), table[0])
        total = two[:part] + (two[part:] + dot(high, table[1]))
        for place, piece in enumerate(pieces(total)):
            result[place, rows, :] = piece
        return 0

    lax.fori_loop(0, width // part, one, 0)


def swap_halves(x):
    return pltpu.roll(x, SUBLANES // 2, x.ndim - 2)


def upper_half(shape):
    return lax.broadcasted_iota(jnp.int32, shape, len(shape) - 2) < SUBLANES // 2


def interleave(first, second):
    upper = upper_half(first.shape)
    return (
        jnp.where(upper, first, swap_halves(second)),
        jnp.where(upper, swap_halves(first), second),
    )


def kernel(
    ranks, columns, observed, gain, trans, dynamics, smooth_gain, filtered, smoothed,
    outbox, forcing, states, drive, results, inbox_f, inbox_s, entries, summed, raw,
    trans_1, trans_p, trans_4, trans_8, smooth_1, smooth_4, smooth_8, dyn_1,
    table_send, table_recv, table_own, force_send, force_recv, filt_send, filt_recv, smoo_send, smoo_recv, own_sem,
):
    steps, tile_width, members = observed.shape
    devices = ranks * columns
    short = steps // 2
    state_width = columns * tile_width
    rank = lax.axis_index("tm")
    column = lax.axis_index("space")
    me = rank * columns + column
    beside = column + 1 - 2 * (column % 2)
    across = (column + 2) % columns

    barrier = pltpu.get_barrier_semaphore()

    def greet(offset, _):
        other = (me + offset) % devices
        pl.semaphore_signal(
            barrier, inc=1, device_id=(other // columns, other % columns), device_id_type=MESH
        )
        return 0

    lax.fori_loop(1, devices, greet, 0)

    sources = (trans, smooth_gain, dynamics)
    for which, source in enumerate(sources):
        pltpu.make_async_copy(source.at[0], raw.at[which, column], table_own.at[which]).start()

    groups = members // SUBLANES

    gain_high, gain_low = pieces(gain[0])

    def force(step, _):
        halves = []
        for half in range(2):
            image = observed[half * short + step].T
            high, low = pieces(image)
            value = dot(high, gain_high) + (dot(low, gain_high) + dot(high, gain_low))
            halves.append(value.reshape(groups, SUBLANES, tile_width))
        even, odd = interleave(*halves)
        outbox[:, 0, pl.ds(step, 1)] = even[:, None]
        outbox[:, 1, pl.ds(step, 1)] = odd[:, None]
        return 0

    lax.fori_loop(0, short, force, 0)
    pl.semaphore_wait(barrier, devices - 1)

    shared = rank % 2
    partner = rank + 1 - 2 * shared

    def half_rows(index):
        count = 3 * tile_width // 2
        return pl.ds(pl.multiple_of(index * count, count), count)

    def table_copy(which, what):
        split = which in SPLIT
        if what == 0:
            place, to = column, (rank, across)
            rows = half_rows(shared) if split else slice(None)
        elif what == 1:
            place, to, rows = column, (rank, beside), slice(None)
        elif what == 2:
            place, to = across, (rank, beside)
            rows = half_rows(shared) if split else slice(None)
        elif what == 3:
            place, to, rows = across, (partner, column), half_rows(shared)
        else:
            place, to, rows = across, (rank, beside), half_rows(1 - shared)
        source = sources[which].at[0, rows] if what < 2 else raw.at[which, place, rows]
        return pltpu.make_async_remote_copy(
            src_ref=source,
            dst_ref=raw.at[which, place, rows],
            send_sem=table_send.at[which, what],
            recv_sem=table_recv.at[which, what],
            device_id=to,
            device_id_type=MESH,
        )

    def send_table(which):
        table_copy(which, 0).start()
        table_copy(which, 1).start()

    def relay_table(which):
        table_copy(which, 0).wait_recv()
        table_copy(which, 2).start()
        if which in SPLIT:
            table_copy(which, 3).start()

    def relay_again(which):
        if which in SPLIT:
            table_copy(which, 3).wait_recv()
            table_copy(which, 4).start()

    def finish_table(which):
        pltpu.make_async_copy(sources[which].at[0], raw.at[which, column], table_own.at[which]).wait()
        table_copy(which, 1).wait_recv()
        table_copy(which, 2).wait_recv()
        if which in SPLIT:
            table_copy(which, 4).wait_recv()

    def build(which, table):
        for tile in range(columns):
            lanes = slice(tile * tile_width, (tile + 1) * tile_width)
            for row in range(columns):
                rows = slice(row * tile_width, (row + 1) * tile_width)
                shift = row - tile + 1
                if 0 <= shift <= 2:
                    block = raw[which, tile, shift * tile_width : (shift + 1) * tile_width, :]
                    for place, piece in enumerate(pieces(block)):
                        table[place, rows, lanes] = piece
                else:
                    for place in range(2):
                        table[place, rows, lanes] = jnp.zeros((tile_width, tile_width), jnp.bfloat16)

    def lane_part(index):
        return pl.ds(pl.multiple_of(index * tile_width, tile_width), tile_width)

    def force_copy(offset):
        other = (me + offset) % devices
        return pltpu.make_async_remote_copy(
            src_ref=outbox.at[other // 2, other % 2],
            dst_ref=forcing.at[:, rank, :, lane_part(column)],
            send_sem=force_send.at[offset],
            recv_sem=force_recv.at[offset],
            device_id=(other // columns, other % columns),
            device_id_type=MESH,
        )

    def result_copy(offset, source, inbox, send, recv):
        other = (me + offset) % devices
        return pltpu.make_async_remote_copy(
            src_ref=source.at[:, other // columns, :, lane_part(other % columns)],
            dst_ref=inbox.at[me // 2, me % 2],
            send_sem=send.at[offset],
            recv_sem=recv.at[offset],
            device_id=(other // columns, other % columns),
            device_id_type=MESH,
        )

    def over_others(act):
        def one(offset, _):
            act(offset)
            return 0

        lax.fori_loop(1, devices, one, 0)

    send_table(0)
    over_others(lambda offset: force_copy(offset).start())
    own_force = pltpu.make_async_copy(
        outbox.at[me // 2, me % 2], forcing.at[:, rank, :, lane_part(column)], own_sem.at[0]
    )
    own_force.start()
    send_table(1)
    send_table(2)

    relay_table(0)
    finish_table(0)
    build(0, trans_1)
    square(trans_1, trans_p)
    square(trans_p, trans_4)
    square(trans_4, trans_8)
    over_others(lambda offset: force_copy(offset).wait_recv())
    own_force.wait()

    relay_table(1)
    rows = ranks * SUBLANES
    whole = (ranks, SUBLANES, state_width)

    def flat(x):
        return x.reshape(rows, state_width)

    def trial(inputs, order, table):
        def one(index, current):
            return times(current, table) + flat(inputs[order(index)])

        return lax.fori_loop(1, short, one, flat(inputs[order(0)]))

    def chain(order, table):
        entries[order(0)] = jnp.zeros((SUBLANES, state_width), jnp.float32)
        entries[order(1)] = summed[order(0)]

        def one(index, current):
            current = times(current, table) + summed[order(index)]
            entries[order(index + 1)] = current
            return current

        lax.fori_loop(1, ranks - 1, one, summed[order(0)])

    def final(inputs, order, table, entry, outputs):
        def one(index, current):
            current = times(current, table) + flat(inputs[order(index)])
            outputs[order(index)] = current.reshape(whole)
            return current

        lax.fori_loop(0, short, one, entry)

    forward = lambda index: index
    upper = upper_half(whole)
    ends = trial(forcing, forward, trans_1)
    halves = ends.reshape(whole)
    summed[...] = times(ends, trans_4).reshape(whole) + swap_halves(halves)
    relay_table(2)
    relay_again(1)
    chain(forward, trans_8)
    first = entries[...]
    second = times(flat(first), trans_4).reshape(whole) + halves
    relay_again(2)
    final(forcing, forward, trans_1, flat(jnp.where(upper, first, swap_halves(second))), states)

    over_others(lambda offset: result_copy(offset, states, inbox_f, filt_send, filt_recv).start())
    own_filtered = pltpu.make_async_copy(
        states.at[:, rank, :, lane_part(column)], inbox_f.at[me // 2, me % 2], own_sem.at[1]
    )
    own_filtered.start()

    finish_table(1)
    build(1, smooth_1)
    square(smooth_1, trans_p)
    square(trans_p, smooth_4)
    square(smooth_4, smooth_8)
    finish_table(2)
    build(2, dyn_1)

    def innovate(step, _):
        value = flat(states[step])
        mixed = times(times(value, dyn_1), smooth_1)
        place = lax.broadcasted_iota(jnp.int32, mixed.shape, 0)
        at_end = jnp.logical_and(place >= rows - SUBLANES // 2, step == short - 1)
        drive[step] = jnp.where(at_end, value, value - mixed).reshape(whole)
        return 0

    lax.fori_loop(0, short, innovate, 0)

    backward = lambda index: short - 1 - index
    heads = trial(drive, backward, smooth_1)
    halves = heads.reshape(whole)
    summed[...] = swap_halves(times(heads, smooth_4).reshape(whole)) + halves
    chain(lambda index: ranks - 1 - index, smooth_8)
    last = entries[...]
    before = times(flat(last), smooth_4).reshape(whole) + swap_halves(halves)
    final(drive, backward, smooth_1, flat(jnp.where(upper, before, swap_halves(last))), results)

    over_others(lambda offset: result_copy(offset, results, inbox_s, smoo_send, smoo_recv).start())
    own_smoothed = pltpu.make_async_copy(
        results.at[:, rank, :, lane_part(column)], inbox_s.at[me // 2, me % 2], own_sem.at[2]
    )
    own_smoothed.start()

    def deliver(inbox, output):
        def one(step, _):
            parts = interleave(inbox[:, 0, step], inbox[:, 1, step])
            for half, part in enumerate(parts):
                output[half * short + step] = part.reshape(members, tile_width).T
            return 0

        lax.fori_loop(0, short, one, 0)

    over_others(lambda offset: result_copy(offset, states, inbox_f, filt_send, filt_recv).wait_recv())
    own_filtered.wait()
    deliver(inbox_f, filtered)
    over_others(lambda offset: result_copy(offset, results, inbox_s, smoo_send, smoo_recv).wait_recv())
    own_smoothed.wait()
    deliver(inbox_s, smoothed)

    for which in range(3):
        for what in range(5 if which in SPLIT else 3):
            table_copy(which, what).wait_send()
    over_others(lambda offset: force_copy(offset).wait_send())
    over_others(lambda offset: result_copy(offset, states, inbox_f, filt_send, filt_recv).wait_send())
    over_others(lambda offset: result_copy(offset, results, inbox_s, smoo_send, smoo_recv).wait_send())


def member_body(ranks, columns, observed, gain, trans, dynamics, smooth_gain):
    steps, tile_width, members = observed.shape
    devices = ranks * columns
    short = steps // 2
    width = columns * tile_width
    pairs = devices // 2
    boxes = pltpu.VMEM((pairs, 2, short, SUBLANES, tile_width), jnp.float32)
    series = pltpu.VMEM((short, ranks, SUBLANES, width), jnp.float32)
    block = pltpu.VMEM((ranks, SUBLANES, width), jnp.float32)
    table = pltpu.VMEM((2, width, width), jnp.bfloat16)
    each = pltpu.SemaphoreType.DMA((devices,))
    vmem = pl.BlockSpec(memory_space=pltpu.VMEM)
    return pl.pallas_call(
        partial(kernel, ranks, columns),
        out_shape=[jax.ShapeDtypeStruct(observed.shape, jnp.float32)] * 2,
        in_specs=[vmem] * 5,
        out_specs=[vmem] * 2,
        scratch_shapes=[
            boxes, series, series, series, series, boxes, boxes, block, block,
            pltpu.VMEM((3, columns, 3 * tile_width, tile_width), jnp.float32),
            table, table, table, table, table, table, table, table,
            pltpu.SemaphoreType.DMA((3, 5)),
            pltpu.SemaphoreType.DMA((3, 5)),
            pltpu.SemaphoreType.DMA((3,)),
            each, each, each, each, each, each,
            pltpu.SemaphoreType.DMA((3,)),
        ],
        compiler_params=pltpu.CompilerParams(
            collective_id=0, has_side_effects=True, vmem_limit_bytes=56 * 2**20
        ),
    )(observed, gain, trans, dynamics, smooth_gain)


def by_members(mesh, observed, gain, trans, dynamics, smooth_gain):
    ranks, columns = mesh.shape["tm"], mesh.shape["space"]
    devices = ranks * columns
    steps, tile_width, members = observed.shape
    fits = (
        members * 2 == devices * SUBLANES
        and steps % 2 == 0
        and columns == 4
        and ranks >= 3
        and tile_width == 128
        and members == 128
    )
    if fits:
        return tuple(member_body(ranks, columns, observed, gain, trans, dynamics, smooth_gain))
    return body(observed, gain, trans, dynamics, smooth_gain)


def solution(mesh):
    return jax.shard_map(
        partial(by_members, mesh),
        mesh=mesh,
        in_specs=(
            P("tm", "space", None),
            P("space", None, None),
            P("space", None, None),
            P("space", None, None),
            P("space", None, None),
        ),
        out_specs=(P("tm", "space", None), P("tm", "space", None)),
        check_vma=False,
    )
```
